128 devices in a mesh: section: 16 (over z_lo, y, core), ep: 8 (over z_hi, x).
Axes of the slice: x: 4, y: 4, z: 4 (z_hi: 2, z_lo: 2; z = z_hi * 2 + z_lo), core: 2. Of those that a mesh axis runs over, the one named last changes fastest.
Arguments:
- fwd_input: bfloat16 [16, 1024, 3584], P('section', 'ep'), may hold values from -6 to 6
- bwd_input: bfloat16 [16, 1024, 3584], P('section', 'ep'), may hold values from -6 to 6
- bwd_grad: bfloat16 [16, 1024, 3584], P('section', 'ep'), may hold values from -6 to 6
- fwd_ids: int32 [16, 1024, 2], P('section', 'ep'), may hold values from 0 to 7, all different within a row; in each aligned block of 128 rows (0 to 127, 128 to 255, ...) at most 48 rows name the same one
- bwd_ids: int32 [16, 1024, 2], P('section', 'ep'), may hold values from 0 to 7, all different within a row; in each aligned block of 128 rows (0 to 127, 128 to 255, ...) at most 48 rows name the same one
- norm_gain: float32 [16, 3584], P('section'), may hold values from 0.5 to 1.5
- router: bfloat16 [16, 3584, 8], P('section'), may hold values from -0.09375 to 0.09375
- gate_w: bfloat16 [16, 8, 3584, 1024], P('section', 'ep'), may hold values from -0.09375 to 0.09375
- up_w: bfloat16 [16, 8, 3584, 1024], P('section', 'ep'), may hold values from -0.09375 to 0.09375
- down_w: bfloat16 [16, 8, 1024, 3584], P('section', 'ep'), may hold values from -0.1875 to 0.1875
Outputs:
- fwd_next: bfloat16 [16, 1024, 3584], P('section', 'ep')
- bwd_prev: bfloat16 [16, 1024, 3584], P('section', 'ep')
The draws below stay inside these ranges and needn't reach their ends.
Inputs may be any that keep to these rules, and one draw needn't show every extreme that they name: `fwd_ids`: each token names 2 different experts of 0 to 7; among the 128 tokens of one index of ep in one section no expert is named more than 48 times, a bound that some block reaches. `bwd_ids`: each token names 2 different experts of 0 to 7; among the 128 tokens of one index of ep in one section no expert is named more than 48 times, a bound that some block reaches.
All inputs are finite; a program needn't handle non-finite values.
Results may differ from the reference program's by a relative error of at most 0.0035.
Values may be sent and summed in bfloat16 or wider, within the bound.
A program may use at most 128 MiB of HBM per device.

```python
import math
import jax
import jax.numpy as jnp
import numpy as np
from jax import lax

D = 3584
F = 1024
TOP = 2
TOK_DEV = 128
SECTIONS = 16
EXPERTS = 8
TOKENS = 1024
CAP = 48
N_EP = 8


def block_scale(stream_key, dims, shards, smallest, largest):
    level = 1.0
    for dim, parts in shards:
        heights = jax.random.uniform(jax.random.fold_in(jax.random.fold_in(stream_key, 6), dim), (parts,), jnp.float32, smallest / len(shards), largest / len(shards))
        level = level * jnp.repeat(jnp.exp(heights), dims[dim] // parts).reshape((-1,) + (1,) * (len(dims) - 1 - dim))
    return level


def deal_out(rng, own, number, rows, amount, top, limit, lean):
    ranking = jax.random.permutation(rng, amount)
    crowded, usual = portions_of(amount, rows * top, limit, lean, True), portions_of(amount, rows * top, limit, lean, False)
    places = jnp.arange(amount)

    def named(tallies, offset_by):
        used = int((tallies > 0).sum())
        fixed = max(1, used // 4)
        shifted = fixed + (places - fixed + offset_by * (used - fixed)) % max(1, amount - fixed)
        return jnp.zeros((amount,), jnp.int32).at[ranking[jnp.where(places < fixed, places, shifted)]].set(jnp.asarray(tallies, jnp.int32))

    tallies = jnp.where(number % 4 == 0, named(crowded, number // 4), named(usual, number - number // 4 - 1))
    mixed = jax.random.permutation(jax.random.fold_in(own, 3), amount)
    source_of, taker = mixed[0:amount // 2 * 2:2], mixed[1:amount // 2 * 2:2]
    slack = jnp.minimum(tallies[source_of] - 1, limit - tallies[taker]) // 2
    slack = jnp.where((source_of == ranking[0]) | (taker == ranking[0]) | (tallies[taker] == 0), 0, jnp.maximum(slack, 0))
    shifted = jax.random.randint(jax.random.fold_in(own, 4), (amount // 2,), 0, 1 << 20) % (slack + 1)
    tallies = tallies.at[source_of].add(-shifted).at[taker].add(shifted)
    items = jnp.searchsorted(jnp.cumsum(tallies), jnp.arange(rows * top), side="right").astype(jnp.int32)
    grid = items.reshape(top, rows).T
    grid = grid[jax.random.permutation(jax.random.fold_in(own, 1), rows)]
    offset_by = jax.random.randint(jax.random.fold_in(own, 2), (rows, 1), 0, top)
    return jnp.take_along_axis(grid, (jnp.arange(top)[None, :] + offset_by) % top, axis=1)


def portions_of(count, total, limit, slope, full):
    portions = [(1 << 20) // math.isqrt(standing ** slope) + 1 for standing in range(1, count + 1)]
    largest = limit if full else min(limit, max(-(-total // count), total * portions[0] // sum(portions)))
    least = 1 if total - largest >= count - 1 else 0
    counts, surplus = [largest] + [least] * (count - 1), total - largest - least * (count - 1)
    while surplus > 0:
        candidates = [i for i in range(1, count) if counts[i] < largest] or [i for i in range(1, count) if counts[i] < limit]
        whole, left = sum([portions[i] for i in candidates]), surplus
        for i in candidates:
            extra = min(limit - counts[i], max(1, left * portions[i] // whole), surplus)
            counts[i] = counts[i] + extra
            surplus = surplus - extra
    return np.array(counts)


def bell_draw(key, shape, deviation, limit, split=(), kind=jnp.bfloat16):
    gain = block_scale(key, shape, split, -0.22, 0.18) if split else 1.0
    values = jax.random.normal(key, shape, jnp.float32) * deviation * gain
    return jnp.minimum(jnp.maximum(values, -limit), limit).astype(kind)


def setup_inputs(seed: int = 0) -> dict:
    seeds = jax.random.split(jax.random.key(seed), 11)
    fwd_input = bell_draw(seeds[0], (SECTIONS, TOKENS, D), 1.0, 6.0, ((0, 16), (1, 8)))
    bwd_input = bell_draw(seeds[1], (SECTIONS, TOKENS, D), 1.0, 6.0, ((0, 16), (1, 8)))
    bwd_grad = bell_draw(seeds[2], (SECTIONS, TOKENS, D), 1.0, 6.0, ((0, 16), (1, 8)))
    fwd_ids_keys = jax.random.split(jax.random.fold_in(seeds[3], 1), SECTIONS * TOKENS // TOK_DEV)
    fwd_ids_turns = jax.random.permutation(jax.random.fold_in(seeds[3], 3), SECTIONS * TOKENS // TOK_DEV)
    fwd_ids = jax.vmap(lambda own, number: deal_out(jax.random.fold_in(seeds[3], 2), own, number, TOK_DEV, EXPERTS, TOP, CAP, 1))(fwd_ids_keys, fwd_ids_turns).reshape((SECTIONS, TOKENS, TOP))
    bwd_ids_keys = jax.random.split(jax.random.fold_in(seeds[4], 1), SECTIONS * TOKENS // TOK_DEV)
    bwd_ids_turns = jax.random.permutation(jax.random.fold_in(seeds[4], 3), SECTIONS * TOKENS // TOK_DEV)
    bwd_ids = jax.vmap(lambda own, number: deal_out(jax.random.fold_in(seeds[4], 2), own, number, TOK_DEV, EXPERTS, TOP, CAP, 1))(bwd_ids_keys, bwd_ids_turns).reshape((SECTIONS, TOKENS, TOP))
    norm_gain = jnp.clip(1.0 + 0.1 * jax.random.normal(seeds[5], (SECTIONS, D), jnp.float32), 0.5, 1.5)
    router = bell_draw(seeds[6], (SECTIONS, D, EXPERTS), D ** -0.5, 0.09375, ((0, 16),))
    gate_w = bell_draw(seeds[7], (SECTIONS, EXPERTS, D, F), D ** -0.5, 0.09375, ((0, 16), (1, 8)))
    up_w = bell_draw(seeds[8], (SECTIONS, EXPERTS, D, F), D ** -0.5, 0.09375, ((0, 16), (1, 8)))
    down_w = bell_draw(seeds[9], (SECTIONS, EXPERTS, F, D), F ** -0.5, 0.1875, ((0, 16), (1, 8)))
    return {"fwd_input": fwd_input, "bwd_input": bwd_input, "bwd_grad": bwd_grad, "fwd_ids": fwd_ids, "bwd_ids": bwd_ids, "norm_gain": norm_gain, "router": router, "gate_w": gate_w, "up_w": up_w, "down_w": down_w}


NORM_EPSILON = 1e-06
ROUTE_SCALE = 2.5

def norm_rows(hidden, gain_vec):
    hidden_f32 = hidden.astype(jnp.float32)
    inverse = lax.rsqrt(lax.optimization_barrier(jnp.mean(hidden_f32 * hidden_f32, axis=1, keepdims=True)) + NORM_EPSILON)
    return ((hidden_f32 * inverse * gain_vec).astype(jnp.bfloat16), inverse)

def routing(normed, router_mat, expert_ids):
    logits = jnp.dot(normed, router_mat, preferred_element_type=jnp.float32)
    scores = jax.nn.sigmoid(logits)
    picked = jnp.take_along_axis(scores, expert_ids, axis=1)
    total_score = lax.optimization_barrier(jnp.sum(picked, axis=1, keepdims=True))
    return (scores, total_score, picked / total_score)

def slot_table(expert_ids, n_experts, slot_room):
    flat_ids = expert_ids.reshape(-1).astype(jnp.int32)
    entry_count = flat_ids.shape[0]
    sort_order = jnp.argsort(flat_ids, stable=True).astype(jnp.int32)
    expert_counts = jax.ops.segment_sum(jnp.ones((entry_count,), jnp.int32), flat_ids, num_segments=n_experts).astype(jnp.int32)
    group_starts = jnp.cumsum(expert_counts).astype(jnp.int32) - expert_counts
    ranks_sorted = jnp.arange(entry_count, dtype=jnp.int32) - group_starts[flat_ids[sort_order]]
    slot_ranks = jnp.zeros((entry_count,), jnp.int32).at[sort_order].set(ranks_sorted)
    slot_index = flat_ids * slot_room + slot_ranks
    slot_owner = jnp.full((n_experts * slot_room,), -1, jnp.int32).at[slot_index].set(jnp.arange(entry_count, dtype=jnp.int32))
    return (slot_index, slot_owner)

def pack_rows(row_data, slot_owner, row_stride):
    slot_valid = slot_owner >= 0
    source_row = jnp.where(slot_valid, slot_owner // row_stride, 0).astype(jnp.int32)
    return jnp.where(slot_valid[:, None], row_data[source_row], jnp.zeros((), row_data.dtype))

def section_step(inputs):
    fwd_h, bwd_h, grad_out, ids_fwd, ids_bwd, gain_vec, router_mat, gate_mats, up_mats, down_mats = inputs
    n_experts = router_mat.shape[1]
    slot_room = N_EP * CAP
    model_width = fwd_h.shape[1]
    token_count = fwd_h.shape[0]
    gate_f32 = gate_mats.astype(jnp.float32)
    up_f32 = up_mats.astype(jnp.float32)
    down_f32 = down_mats.astype(jnp.float32)

    def forward(hidden, expert_ids):
        normed, inverse = norm_rows(hidden, gain_vec)
        scores, total_score, weights = routing(normed, router_mat, expert_ids)
        slot_index, slot_owner = slot_table(expert_ids, n_experts, slot_room)
        expert_rows = pack_rows(normed, slot_owner, TOP).reshape(n_experts, slot_room, model_width)
        rows_f32 = expert_rows.astype(jnp.float32)
        gate_val = jnp.einsum('erd,edf->erf', rows_f32, gate_f32)
        up_val = jnp.einsum('erd,edf->erf', rows_f32, up_f32)
        active = (jax.nn.silu(gate_val) * up_val).astype(jnp.bfloat16)
        output = jnp.einsum('erf,efd->erd', active.astype(jnp.float32), down_f32).astype(jnp.bfloat16)
        picked_rows = output.reshape(-1, model_width)[slot_index].reshape(token_count, TOP, model_width)
        mixed = hidden.astype(jnp.float32) + ROUTE_SCALE * lax.optimization_barrier(jnp.sum(weights[:, :, None] * picked_rows.astype(jnp.float32), axis=1))
        return (mixed.astype(jnp.bfloat16), (normed, inverse, scores, total_score, weights, slot_index, slot_owner, gate_val, up_val, picked_rows))
    mixed_fwd, _ = forward(fwd_h, ids_fwd)
    _, saved = forward(bwd_h, ids_bwd)
    normed, inverse, scores, total_score, weights, slot_index, slot_owner, gate_val, up_val, picked_rows = saved
    grad_top = grad_out.astype(jnp.float32)
    d_weights = ROUTE_SCALE * lax.optimization_barrier(jnp.sum(grad_top[:, None, :] * picked_rows.astype(jnp.float32), axis=2))
    d_rows = (ROUTE_SCALE * weights[:, :, None] * grad_top[:, None, :]).astype(jnp.bfloat16)
    packed_grads = pack_rows(d_rows.reshape(token_count * TOP, model_width), slot_owner, 1)
    grads_f32 = packed_grads.reshape(n_experts, slot_room, model_width).astype(jnp.float32)
    d_active = jnp.einsum('erd,efd->erf', grads_f32, down_f32)
    gate_sigmoid = jax.nn.sigmoid(gate_val)
    d_gate = (d_active * up_val * gate_sigmoid * (1.0 + gate_val * (1.0 - gate_sigmoid))).astype(jnp.bfloat16)
    d_up = (d_active * gate_val * gate_sigmoid).astype(jnp.bfloat16)
    d_gate_f32 = d_gate.astype(jnp.float32)
    d_up_f32 = d_up.astype(jnp.float32)
    d_back = (jnp.einsum('erf,edf->erd', d_gate_f32, gate_f32) + jnp.einsum('erf,edf->erd', d_up_f32, up_f32)).astype(jnp.bfloat16)
    d_normed = lax.optimization_barrier(jnp.sum(d_back.reshape(-1, model_width)[slot_index].reshape(token_count, TOP, model_width).astype(jnp.float32), axis=1))
    d_picked = (d_weights - lax.optimization_barrier(jnp.sum(d_weights * weights, axis=1, keepdims=True))) / total_score
    token_index = jnp.arange(token_count, dtype=jnp.int32)[:, None]
    d_scores = jnp.zeros_like(scores).at[token_index, ids_bwd].add(d_picked)
    d_logits = (d_scores * scores * (1.0 - scores)).astype(jnp.bfloat16)
    d_normed = d_normed + jnp.dot(d_logits, router_mat.T, preferred_element_type=jnp.float32)
    hidden_f32 = bwd_h.astype(jnp.float32)
    scaled = gain_vec * d_normed
    d_hidden = inverse * scaled - hidden_f32 * inverse * inverse * inverse * lax.optimization_barrier(jnp.sum(scaled * hidden_f32, axis=1, keepdims=True)) / model_width
    d_input = (grad_top + d_hidden).astype(jnp.bfloat16)
    return (mixed_fwd, d_input)

def reference(fwd_input, bwd_input, bwd_grad, fwd_ids, bwd_ids, norm_gain, router, gate_w, up_w, down_w):
    mixed, d_input = lax.map(section_step, (fwd_input, bwd_input, bwd_grad, fwd_ids, bwd_ids, norm_gain, router, gate_w, up_w, down_w))
    fwd_next = jnp.roll(mixed, 1, axis=0)
    bwd_prev = jnp.roll(d_input, -1, axis=0)
    return (fwd_next, bwd_prev)
```

```python
import jax
import jax.numpy as jnp
from jax import lax
from jax.experimental import pallas as pl
from jax.experimental.pallas import tpu as pltpu
from jax.sharding import PartitionSpec as P

NORM_EPSILON = 1e-06
ROUTE_SCALE = 2.5

D = 3584
F = 1024
T = 128
E = 8
CAP = 48
S = E * CAP
NEP = 8
NSEC = 16
MODES = (0, 1, 0)
BACK_ORDER = ((0, 1), (1, 0), (1, -1), (1, 1), (0, 2), (1, 2), (0, -1))
OUT_ORDER = ((0, 1), (1, 0), (0, -1), (1, 1), (0, 2), (1, -1), (1, 2))

BACK_CHUNKS = 7
BACK_WIDTH = D // BACK_CHUNKS
OUT_CHUNKS = 4
OUT_WIDTH = D // OUT_CHUNKS

HAND_PARTS = 4

MESH = pl.DeviceIdType.MESH
F32 = jnp.float32
BF16 = jnp.bfloat16


def dot(a, b):
    return jnp.dot(a, b, preferred_element_type=F32)


def dot_t(a, b):
    return lax.dot_general(a, b, (((1,), (1,)), ((), ())), preferred_element_type=F32)


def cols(i, width):
    return pl.ds(pl.multiple_of(i * width, 128), width)


def block(i):
    return pl.ds(pl.multiple_of(i * CAP, 16), CAP)


def kernel(
    ids_f, ids_b, gain, router, hf_hbm, hb_hbm, g_hbm, gate_hbm, up_hbm, down_hbm,
    outf_hbm, outb_hbm,
    gate, up, down, hf, hb, g,
    send, recv, raw, retb, retf, norm, pmat, qmat, scale, wmat_b, wmat_f,
    dact, dab, act, dacc, dots, dotr, u, stage_f, stage_b, inv, small, idx, share,
    wsem, isem, xsem_s, xsem_r, rsem_s, rsem_r, dsem_s, dsem_r, bsem_s, bsem_r, tsem_s, tsem_r,
    fsem_s, fsem_r, pf_s, pf_r, pb_s, pb_r,
):
    sec = lax.axis_index("section")
    me = lax.axis_index("ep")
    mx, mz = lax.rem(me, 4), me // 4
    side = 1 - 2 * lax.rem(sec, 2)

    def at_place(dz, dx):
        return lax.rem(mz + dz, 2) * 4 + lax.rem(mx + dx + 4, 4)

    back_peers = [at_place(dz, side * dx) for dz, dx in BACK_ORDER]
    out_peers = [at_place(dz, side * dx) for dz, dx in OUT_ORDER]
    across = at_place(1, 0)
    onward, source = at_place(0, side), at_place(0, -side)
    ahead, behind = lax.rem(sec + 1, NSEC), lax.rem(sec + NSEC - 1, NSEC)

    barrier = pltpu.get_barrier_semaphore()
    for e in back_peers:
        pl.semaphore_signal(barrier, 1, device_id={"ep": e}, device_id_type=MESH)
    for s in (ahead, behind):
        pl.semaphore_signal(barrier, 1, device_id={"section": s}, device_id_type=MESH)

    loads = [
        pltpu.make_async_copy(src, dst, isem.at[i])
        for i, (src, dst) in enumerate(((hb_hbm, hb), (g_hbm, g), (hf_hbm, hf)))
    ]
    weights = [
        pltpu.make_async_copy(src, dst, wsem.at[i])
        for i, (src, dst) in enumerate(((down_hbm, down), (gate_hbm, gate), (up_hbm, up)))
    ]
    for c in (loads[1], loads[0], loads[2]):
        c.start()

    def remote(src, dst, ssem, rsem, e):
        return pltpu.make_async_remote_copy(
            src_ref=src, dst_ref=dst, send_sem=ssem, recv_sem=rsem,
            device_id={"ep": e}, device_id_type=MESH,
        )

    row16 = lax.broadcasted_iota(jnp.int32, (16, T), 0)
    slot48 = lax.broadcasted_iota(jnp.int32, (CAP, T), 0).astype(F32)
    eye48 = (
        lax.broadcasted_iota(jnp.int32, (CAP, T), 0) == lax.broadcasted_iota(jnp.int32, (CAP, T), 1)
    ).astype(F32)
    earlier = (
        lax.broadcasted_iota(jnp.int32, (T, T), 0) < lax.broadcasted_iota(jnp.int32, (T, T), 1)
    ).astype(BF16)

    def places(ids0, ids1, order):
        eid = jnp.full((16, T), -1, jnp.int32)
        for k, e in enumerate(order):
            eid = jnp.where(row16 == k, e, eid)
        named = ((ids0 == eid) | (ids1 == eid)).astype(F32)
        rank = dot(named.astype(BF16), earlier)
        return eid, [
            jnp.where((slot48 == rank[k:k + 1, :]) & (named[k:k + 1, :] > 0.5), 1.0, 0.0)
            for k in range(len(order))
        ]

    def weighted(placed, ids0, ids1, eid, w0, w1):
        per = jnp.where(ids0 == eid, w0, 0.0) + jnp.where(ids1 == eid, w1, 0.0)
        return [p * per[k:k + 1, :] for k, p in enumerate(placed)]

    def pack(flow, half, owner, ids0, ids1, order, rows, w=None):
        eid, placed = places(ids0, ids1, order)
        qmat[...] = jnp.concatenate(placed, axis=0).astype(BF16)
        if w is not None:
            per = jnp.concatenate(weighted(placed, ids0, ids1, eid, w[0], w[1]), axis=0)
            scale[...] = jnp.broadcast_to(jnp.sum(per, axis=1, keepdims=True), (4 * CAP, 128))

        def step(i, c):
            at = cols(i, 512)
            packed = dot(qmat[...], rows[:, at])
            if w is not None:
                packed = scale[:, 0:1] * packed
            packed = packed.astype(BF16)
            recv[flow, block(owner), at] = packed[0:CAP]
            send[flow, half * 3 * CAP:(half + 1) * 3 * CAP, at] = packed[CAP:4 * CAP]
            return c

        lax.fori_loop(0, D // 512, step, 0)

    def launch(flow, half, owner, order):
        for k, e in enumerate(order[1:]):
            remote(
                send.at[flow, pl.ds((half * 3 + k) * CAP, CAP)], recv.at[flow, block(owner)],
                dsem_s.at[flow], dsem_r.at[flow], e,
            ).start()

    def packed_all(flow):
        part = pl.ds(0, 6 * CAP)
        return remote(
            send.at[flow, part], recv.at[flow, part], dsem_s.at[flow], dsem_r.at[flow], across
        )

    def forward_raw(flow, rows, e):
        return remote(rows, raw.at[flow], rsem_s.at[flow], rsem_r.at[flow], e)

    def normalize(rows, into, keep):
        def step(i, c):
            at = pl.ds(pl.multiple_of(i * 16, 16), 16)
            x = rows[at, :].astype(F32)
            r = lax.rsqrt(jnp.mean(x * x, axis=1, keepdims=True) + NORM_EPSILON)
            if keep is not None:
                keep[at, :] = jnp.broadcast_to(r, (16, 128))
            into[at, :] = (x * r * gain[...]).astype(BF16)
            return c

        lax.fori_loop(0, T // 16, step, 0)

    expert8 = lax.broadcasted_iota(jnp.int32, (E, T), 0)

    def route(ids, rows):
        scores = jax.nn.sigmoid(dot_t(router[...], rows[...]))
        s0 = jnp.sum(jnp.where(expert8 == ids[0:1, :], scores, 0.0), axis=0, keepdims=True)
        s1 = jnp.sum(jnp.where(expert8 == ids[1:2, :], scores, 0.0), axis=0, keepdims=True)
        total = s0 + s1
        return scores, s0 / total, s1 / total

    by_plane = [me, at_place(0, 1), at_place(0, 3), at_place(0, 2)]
    by_column = [me, at_place(0, -side), across, at_place(1, -side)]
    relayed = [me, at_place(0, side), across, at_place(1, side)]
    target = [onward if m else across for m in MODES]
    origin = [source if m else across for m in MODES]
    direct = [by_column if m else by_plane for m in MODES]
    relay = [relayed if m else by_plane for m in MODES]
    if MODES[2] == 0:
        relay[2] = [me, at_place(0, -1), at_place(0, 1), at_place(0, 2)]

    ids_copies = [
        remote(ids_b, idx.at[0], xsem_s.at[0], xsem_r.at[0], target[0]),
        remote(ids_b, idx.at[1], xsem_s.at[1], xsem_r.at[1], target[1]),
        remote(ids_f, idx.at[2], xsem_s.at[2], xsem_r.at[2], target[2]),
    ]
    share_copy = remote(share.at[0], share.at[1], xsem_s.at[3], xsem_r.at[3], target[1])

    pl.semaphore_wait(barrier, 9)
    raw_g = forward_raw(1, g, target[1])
    raw_b = forward_raw(0, norm.at[0], target[0])
    raw_f = forward_raw(2, norm.at[1], target[2])
    loads[1].wait()
    raw_g.start()
    for c in ids_copies:
        c.start()
    loads[0].wait()
    normalize(hb, norm.at[0], inv)
    raw_b.start()
    b0, b1 = ids_b[0:1, :], ids_b[1:2, :]
    f0, f1 = ids_f[0:1, :], ids_f[1:2, :]
    pack(0, 0, me, b0, b1, direct[0], norm.at[0])
    launch(0, 0, me, direct[0])
    for c in weights:
        c.start()

    scores, w0, w1 = route(ids_b, norm.at[0])
    small[0] = scores
    small[1] = jnp.broadcast_to(w0, (E, T))
    small[2] = jnp.broadcast_to(w1, (E, T))
    share[0, 0:1, :] = ROUTE_SCALE * w0
    share[0, 1:2, :] = ROUTE_SCALE * w1
    share_copy.start()
    pack(1, 0, me, b0, b1, direct[1], g, (ROUTE_SCALE * w0, ROUTE_SCALE * w1))
    launch(1, 0, me, direct[1])

    loads[2].wait()
    normalize(hf, norm.at[1], None)

    ids_copies[1].wait_recv()
    share_copy.wait_recv()
    raw_g.wait_recv()
    pack(
        1, 1, origin[1], idx[1, 0:1, :], idx[1, 1:2, :], relay[1], raw.at[1],
        (share[1, 0:1, :], share[1, 1:2, :]),
    )
    launch(1, 1, origin[1], relay[1])

    pack(2, 0, me, f0, f1, direct[2], norm.at[1])
    _, w0, w1 = route(ids_f, norm.at[1])
    eid, placed = places(f0, f1, list(range(E)))
    w = jnp.transpose(jnp.concatenate(
        weighted(placed, f0, f1, eid, ROUTE_SCALE * w0, ROUTE_SCALE * w1), axis=0
    ))
    hi = w.astype(BF16)
    wmat_f[0:T, :] = hi
    wmat_f[T:2 * T, :] = (w - hi.astype(F32)).astype(BF16)
    _, placed = places(b0, b1, list(range(E)))
    placed = jnp.concatenate(placed, axis=0)
    pmat[...] = placed.astype(BF16)
    wmat_b[...] = jnp.transpose(placed).astype(BF16)

    ids_copies[0].wait_recv()
    raw_b.wait_recv()
    pack(0, 1, origin[0], idx[0, 0:1, :], idx[0, 1:2, :], relay[0], raw.at[0])
    launch(0, 1, origin[0], relay[0])

    raw_f.start()
    launch(2, 0, me, direct[2])

    for c in weights:
        c.wait()
    packed_all(1).wait_recv()

    def d_act(i, c):
        at = cols(i, 256)
        dact[:, at] = dot_t(recv[1], down[pl.ds(pl.multiple_of(i * 256, 256), 256), :])
        return c

    lax.fori_loop(0, F // 256, d_act, 0)
    packed_all(0).wait_recv()
    dacc[...] = jnp.zeros_like(dacc)

    def hidden_grad(i, c):
        at = cols(i, 256)
        a = dot(recv[0], gate[:, at])
        b = dot(recv[0], up[:, at])
        da = dact[:, at]
        sg = jax.nn.sigmoid(a)
        silu = a * sg
        live = silu * b * da
        dacc[...] += live[:, 0:128] + live[:, 128:256]
        dab[:, at] = (da * b * sg * (1.0 + a * (1.0 - sg))).astype(BF16)
        dab[:, pl.ds(pl.multiple_of(F + i * 256, 128), 256)] = (da * silu).astype(BF16)
        return c

    lax.fori_loop(0, F // 256, hidden_grad, 0)

    ids_copies[2].wait_recv()
    raw_f.wait_recv()
    pack(2, 1, origin[2], idx[2, 0:1, :], idx[2, 1:2, :], relay[2], raw.at[2])
    launch(2, 1, origin[2], relay[2])

    for e in range(E):
        column = jnp.sum(dacc[e * CAP:(e + 1) * CAP, :], axis=1, keepdims=True)
        dots[e] = jnp.broadcast_to(jnp.sum(column * eye48, axis=0, keepdims=True), (E, T))
    for e in back_peers:
        remote(dots.at[e], dotr.at[me], tsem_s, tsem_r, e).start()
    dotr[me] = dots[me]

    def d_rows(i, c):
        at = pl.ds(pl.multiple_of(i * 256, 256), 256)
        recv[0, :, cols(i, 256)] = (
            dot_t(dab[:, 0:F], gate[at, :]) + dot_t(dab[:, F:2 * F], up[at, :])
        ).astype(BF16)
        return c

    for chunk in range(BACK_CHUNKS):
        each = BACK_WIDTH // 256
        lax.fori_loop(chunk * each, (chunk + 1) * each, d_rows, 0)
        at = pl.ds(chunk * BACK_WIDTH, BACK_WIDTH)
        for e in back_peers:
            remote(
                recv.at[0, block(e), at], retb.at[block(me), at],
                bsem_s.at[chunk], bsem_r.at[chunk], e,
            ).start()
        retb[block(me), at] = recv[0, block(me), at]

    packed_all(2).wait_recv()

    def hidden(i, c):
        at = cols(i, 256)
        a = dot(recv[2], gate[:, at])
        b = dot(recv[2], up[:, at])
        act[:, at] = (a * jax.nn.sigmoid(a) * b).astype(BF16)
        return c

    lax.fori_loop(0, F // 256, hidden, 0)

    for chunk in range(OUT_CHUNKS):
        at = pl.ds(chunk * OUT_WIDTH, OUT_WIDTH)
        recv[1, :, at] = dot(act[...], down[:, at]).astype(BF16)
        for e in out_peers:
            remote(
                recv.at[1, block(e), at], retf.at[block(me), at],
                fsem_s.at[chunk], fsem_r.at[chunk], e,
            ).start()
        retf[block(me), at] = recv[1, block(me), at]

    seven = pl.ds(0, 7 * CAP)
    all_dots = remote(dots.at[pl.ds(0, 7)], dotr.at[pl.ds(0, 7)], tsem_s, tsem_r, across)
    all_dots.wait_recv()
    scores = small[0]
    w0, w1 = small[1, 0:1, :], small[2, 0:1, :]
    d0 = jnp.zeros((1, T), F32)
    d1 = jnp.zeros((1, T), F32)
    for e in range(E):
        column = jnp.sum(dotr[e, 0:1, :] * eye48, axis=1, keepdims=True)
        value = jnp.sum(
            pmat[e * CAP:(e + 1) * CAP, :].astype(F32) * column, axis=0, keepdims=True
        )
        d0 = d0 + jnp.where(b0 == e, value, 0.0)
        d1 = d1 + jnp.where(b1 == e, value, 0.0)
    mean = d0 + d1
    d_logits = (
        jnp.where(expert8 == b0, d0 - w0 * mean, 0.0) + jnp.where(expert8 == b1, d1 - w1 * mean, 0.0)
    ) * (1.0 - scores)
    d_logits = jnp.transpose(
        jnp.concatenate([d_logits, jnp.zeros((T - E, T), F32)], axis=0)
    )[:, 0:E].astype(BF16)

    def all_back(chunk):
        at = pl.ds(chunk * BACK_WIDTH, BACK_WIDTH)
        return remote(
            recv.at[0, seven, at], retb.at[seven, at], bsem_s.at[chunk], bsem_r.at[chunk], across
        )

    def all_out(chunk):
        at = pl.ds(chunk * OUT_WIDTH, OUT_WIDTH)
        return remote(
            recv.at[1, seven, at], retf.at[seven, at], fsem_s.at[chunk], fsem_r.at[chunk], across
        )

    total_uh = jnp.zeros((T, 1), F32)
    for chunk in range(BACK_CHUNKS):
        all_back(chunk).wait_recv()
        for part in range(1):
            at = pl.ds(chunk * BACK_WIDTH + part * BACK_WIDTH, BACK_WIDTH)
            d_normed = dot(wmat_b[...], retb[:, at]) + dot(d_logits, router[:, at])
            scaled = gain[:, at] * d_normed
            u[:, at] = scaled
            total_uh = total_uh + jnp.sum(scaled * hb[:, at].astype(F32), axis=1, keepdims=True)
    r = inv[:, 0:1]
    pull = r * r * r * total_uh * (1.0 / D)

    def next_copy(at, out, stage, ssem, rsem, target):
        return pltpu.make_async_remote_copy(
            src_ref=stage.at[:, at], dst_ref=out.at[:, at], send_sem=ssem, recv_sem=rsem,
            device_id={"section": target}, device_id_type=MESH,
        )

    for chunk in range(OUT_CHUNKS):
        at = pl.ds(chunk * OUT_WIDTH, OUT_WIDTH)
        stage_b[:, at] = (
            g[:, at].astype(F32) + r * u[:, at] - hb[:, at].astype(F32) * pull
        ).astype(BF16)
        next_copy(at, outb_hbm, stage_b, pb_s, pb_r, behind).start()

    for chunk in range(OUT_CHUNKS):
        at = pl.ds(chunk * OUT_WIDTH, OUT_WIDTH)
        all_out(chunk).wait_recv()
        both = dot(wmat_f[...], retf[:, at])
        stage_f[:, at] = (hf[:, at].astype(F32) + (both[0:T] + both[T:2 * T])).astype(BF16)
        next_copy(at, outf_hbm, stage_f, pf_s, pf_r, ahead).start()

    for c in [*ids_copies, share_copy, raw_g, raw_b, raw_f, all_dots]:
        c.wait_send()
    for flow in range(3):
        packed_all(flow).wait_send()
    for chunk in range(BACK_CHUNKS):
        all_back(chunk).wait_send()
    for chunk in range(OUT_CHUNKS):
        all_out(chunk).wait_send()
    every = pl.ds(0, D)
    next_copy(every, outb_hbm, stage_b, pb_s, pb_r, behind).wait()
    next_copy(every, outf_hbm, stage_f, pf_s, pf_r, ahead).wait()


def hand_over(a_in, b_in, a_out, b_out, held, isem, osem):
    rows = T // HAND_PARTS
    pairs = [
        (src.at[pl.ds(i * rows, rows)], dst.at[pl.ds(i * rows, rows)])
        for i in range(HAND_PARTS)
        for src, dst in ((a_in, a_out), (b_in, b_out))
    ]
    ins = [pltpu.make_async_copy(s, held.at[i], isem.at[i]) for i, (s, _) in enumerate(pairs)]
    outs = [pltpu.make_async_copy(held.at[i], d, osem.at[i]) for i, (_, d) in enumerate(pairs)]
    for c in ins:
        c.start()
    for i, c in enumerate(outs):
        ins[i].wait()
        c.start()
    for c in outs:
        c.wait()


def local(
    fwd_input, bwd_input, bwd_grad, fwd_ids, bwd_ids, norm_gain, router, gate_w, up_w, down_w
):
    vmem = pl.BlockSpec(memory_space=pltpu.VMEM)
    hbm = pl.BlockSpec(memory_space=pl.ANY)
    dma = pltpu.SemaphoreType.DMA
    out = jax.ShapeDtypeStruct((T, D), BF16)
    fwd_next, bwd_prev = pl.pallas_call(
        kernel,
        out_shape=(out, out),
        in_specs=[vmem] * 4 + [hbm] * 6,
        out_specs=(hbm, hbm),
        scratch_shapes=[
            pltpu.VMEM((D, F), BF16), pltpu.VMEM((D, F), BF16), pltpu.VMEM((F, D), BF16),
            pltpu.VMEM((T, D), BF16), pltpu.VMEM((T, D), BF16), pltpu.VMEM((T, D), BF16),
            pltpu.VMEM((3, 6 * CAP, D), BF16), pltpu.VMEM((3, S, D), BF16), pltpu.VMEM((3, T, D), BF16),
            pltpu.VMEM((S, D), BF16), pltpu.VMEM((S, D), BF16), pltpu.VMEM((2, T, D), BF16),
            pltpu.VMEM((S, T), BF16), pltpu.VMEM((4 * CAP, T), BF16), pltpu.VMEM((4 * CAP, 128), F32),
            pltpu.VMEM((T, S), BF16), pltpu.VMEM((2 * T, S), BF16),
            pltpu.VMEM((S, F), F32), pltpu.VMEM((S, 2 * F), BF16), pltpu.VMEM((S, F), BF16),
            pltpu.VMEM((S, 128), F32), pltpu.VMEM((E, E, T), F32), pltpu.VMEM((E, E, T), F32),
            pltpu.VMEM((T, D), F32), pltpu.VMEM((T, D), BF16), pltpu.VMEM((T, D), BF16),
            pltpu.VMEM((T, 128), F32), pltpu.VMEM((3, E, T), F32),
            pltpu.VMEM((3, 2, T), jnp.int32), pltpu.VMEM((2, E, T), F32),
            dma((3,)), dma((3,)), dma((4,)), dma((4,)), dma((3,)), dma((3,)), dma((3,)), dma((3,)),
            dma((BACK_CHUNKS,)), dma((BACK_CHUNKS,)), dma, dma,
            dma((OUT_CHUNKS,)), dma((OUT_CHUNKS,)), dma, dma, dma, dma,
        ],
        compiler_params=pltpu.CompilerParams(
            collective_id=0, has_side_effects=True, vmem_limit_bytes=67043328
        ),
    )(
        fwd_ids[0].T, bwd_ids[0].T, norm_gain, router[0].T,
        fwd_input[0], bwd_input[0], bwd_grad[0], gate_w[0, 0], up_w[0, 0], down_w[0, 0],
    )
    parts = 2 * HAND_PARTS
    fwd_next, bwd_prev = pl.pallas_call(
        hand_over,
        out_shape=(out, out),
        in_specs=[hbm, hbm],
        out_specs=(hbm, hbm),
        scratch_shapes=[
            pltpu.VMEM((parts, T // HAND_PARTS, D), BF16), dma((parts,)), dma((parts,)),
        ],
    )(fwd_next, bwd_prev)
    return (fwd_next[None], bwd_prev[None])


def solution(mesh):
    placed = (
        P("section", "ep", None),
        P("section", "ep", None),
        P("section", "ep", None),
        P("section", "ep", None),
        P("section", "ep", None),
        P("section", None),
        P("section", None, None),
        P("section", "ep", None, None),
        P("section", "ep", None, None),
        P("section", "ep", None, None),
    )
    return jax.shard_map(
        local,
        mesh=mesh,
        in_specs=placed,
        out_specs=(P("section", "ep", None), P("section", "ep", None)),
        check_vma=False,
    )
```

```python
import jax
import jax.numpy as jnp
from jax import lax
from jax.experimental import pallas as pl
from jax.experimental.pallas import tpu as pltpu
from jax.sharding import PartitionSpec as P

NORM_EPSILON = 1e-06
ROUTE_SCALE = 2.5

D = 3584
F = 1024
T = 128
E = 8
CAP = 48
S = E * CAP
NEP = 8
NSEC = 16
MODES = (0, 1, 0)
BACK_ORDER = ((0, 2), (1, 0), (1, -1), (1, 1), (0, 1), (1, 2), (0, -1))
OUT_ORDER = ((0, 1), (1, 0), (0, -1), (1, 1), (0, 2), (1, -1), (1, 2))

BACK_CHUNKS = 7
BACK_WIDTH = D // BACK_CHUNKS
OUT_CHUNKS = 4
OUT_WIDTH = D // OUT_CHUNKS

HAND_PARTS = 4

MESH = pl.DeviceIdType.MESH
F32 = jnp.float32
BF16 = jnp.bfloat16


def dot(a, b):
    return jnp.dot(a, b, preferred_element_type=F32)


def dot_t(a, b):
    return lax.dot_general(a, b, (((1,), (1,)), ((), ())), preferred_element_type=F32)


def cols(i, width):
    return pl.ds(pl.multiple_of(i * width, 128), width)


def block(i):
    return pl.ds(pl.multiple_of(i * CAP, 16), CAP)


def kernel(
    ids_f, ids_b, gain, router, hf_hbm, hb_hbm, g_hbm, gate_hbm, up_hbm, down_hbm,
    outf_hbm, outb_hbm,
    gate, up, down, hf, hb, g,
    send, recv, raw, retb, retf, norm, pmat, qmat, scale, wmat_b, wmat_f,
    dact, dab, act, dacc, dots, dotr, u, stage_f, stage_b, inv, small, idx, share,
    wsem, isem, xsem_s, xsem_r, rsem_s, rsem_r, dsem_s, dsem_r, bsem_s, bsem_r, tsem_s, tsem_r,
    fsem_s, fsem_r, pf_s, pf_r, pb_s, pb_r,
):
    sec = lax.axis_index("section")
    me = lax.axis_index("ep")
    mx, mz = lax.rem(me, 4), me // 4
    side = 1 - 2 * lax.rem(sec, 2)

    def at_place(dz, dx):
        return lax.rem(mz + dz, 2) * 4 + lax.rem(mx + dx + 4, 4)

    back_peers = [at_place(dz, side * dx) for dz, dx in BACK_ORDER]
    out_peers = [at_place(dz, side * dx) for dz, dx in OUT_ORDER]
    across = at_place(1, 0)
    onward, source = at_place(0, side), at_place(0, -side)
    ahead, behind = lax.rem(sec + 1, NSEC), lax.rem(sec + NSEC - 1, NSEC)

    barrier = pltpu.get_barrier_semaphore()
    for e in back_peers:
        pl.semaphore_signal(barrier, 1, device_id={"ep": e}, device_id_type=MESH)
    for s in (ahead, behind):
        pl.semaphore_signal(barrier, 1, device_id={"section": s}, device_id_type=MESH)

    loads = [
        pltpu.make_async_copy(src, dst, isem.at[i])
        for i, (src, dst) in enumerate(((hb_hbm, hb), (g_hbm, g), (hf_hbm, hf)))
    ]
    weights = [
        pltpu.make_async_copy(src, dst, wsem.at[i])
        for i, (src, dst) in enumerate(((down_hbm, down), (gate_hbm, gate), (up_hbm, up)))
    ]
    for c in (loads[1], loads[0], loads[2]):
        c.start()

    def remote(src, dst, ssem, rsem, e):
        return pltpu.make_async_remote_copy(
            src_ref=src, dst_ref=dst, send_sem=ssem, recv_sem=rsem,
            device_id={"ep": e}, device_id_type=MESH,
        )

    row16 = lax.broadcasted_iota(jnp.int32, (16, T), 0)
    slot48 = lax.broadcasted_iota(jnp.int32, (CAP, T), 0).astype(F32)
    eye48 = (
        lax.broadcasted_iota(jnp.int32, (CAP, T), 0) == lax.broadcasted_iota(jnp.int32, (CAP, T), 1)
    ).astype(F32)
    earlier = (
        lax.broadcasted_iota(jnp.int32, (T, T), 0) < lax.broadcasted_iota(jnp.int32, (T, T), 1)
    ).astype(BF16)

    def places(ids0, ids1, order):
        eid = jnp.full((16, T), -1, jnp.int32)
        for k, e in enumerate(order):
            eid = jnp.where(row16 == k, e, eid)
        named = ((ids0 == eid) | (ids1 == eid)).astype(F32)
        rank = dot(named.astype(BF16), earlier)
        return eid, [
            jnp.where((slot48 == rank[k:k + 1, :]) & (named[k:k + 1, :] > 0.5), 1.0, 0.0)
            for k in range(len(order))
        ]

    def weighted(placed, ids0, ids1, eid, w0, w1):
        per = jnp.where(ids0 == eid, w0, 0.0) + jnp.where(ids1 == eid, w1, 0.0)
        return [p * per[k:k + 1, :] for k, p in enumerate(placed)]

    def pack(flow, half, owner, ids0, ids1, order, rows, w=None):
        eid, placed = places(ids0, ids1, order)
        qmat[...] = jnp.concatenate(placed, axis=0).astype(BF16)
        if w is not None:
            per = jnp.concatenate(weighted(placed, ids0, ids1, eid, w[0], w[1]), axis=0)
            scale[...] = jnp.broadcast_to(jnp.sum(per, axis=1, keepdims=True), (4 * CAP, 128))

        def step(i, c):
            at = cols(i, 512)
            packed = dot(qmat[...], rows[:, at])
            if w is not None:
                packed = scale[:, 0:1] * packed
            packed = packed.astype(BF16)
            recv[flow, block(owner), at] = packed[0:CAP]
            send[flow, half * 3 * CAP:(half + 1) * 3 * CAP, at] = packed[CAP:4 * CAP]
            return c

        lax.fori_loop(0, D // 512, step, 0)

    def launch(flow, half, owner, order):
        for k, e in enumerate(order[1:]):
            remote(
                send.at[flow, pl.ds((half * 3 + k) * CAP, CAP)], recv.at[flow, block(owner)],
                dsem_s.at[flow], dsem_r.at[flow], e,
            ).start()

    def packed_all(flow):
        part = pl.ds(0, 6 * CAP)
        return remote(
            send.at[flow, part], recv.at[flow, part], dsem_s.at[flow], dsem_r.at[flow], across
        )

    def forward_raw(flow, rows, e):
        return remote(rows, raw.at[flow], rsem_s.at[flow], rsem_r.at[flow], e)

    def normalize(rows, into, keep):
        def step(i, c):
            at = pl.ds(pl.multiple_of(i * 16, 16), 16)
            x = rows[at, :].astype(F32)
            r = lax.rsqrt(jnp.mean(x * x, axis=1, keepdims=True) + NORM_EPSILON)
            if keep is not None:
                keep[at, :] = jnp.broadcast_to(r, (16, 128))
            into[at, :] = (x * r * gain[...]).astype(BF16)
            return c

        lax.fori_loop(0, T // 16, step, 0)

    expert8 = lax.broadcasted_iota(jnp.int32, (E, T), 0)

    def route(ids, rows):
        scores = jax.nn.sigmoid(dot_t(router[...], rows[...]))
        s0 = jnp.sum(jnp.where(expert8 == ids[0:1, :], scores, 0.0), axis=0, keepdims=True)
        s1 = jnp.sum(jnp.where(expert8 == ids[1:2, :], scores, 0.0), axis=0, keepdims=True)
        total = s0 + s1
        return scores, s0 / total, s1 / total

    by_plane = [me, at_place(0, 1), at_place(0, 3), at_place(0, 2)]
    by_column = [me, at_place(0, -side), across, at_place(1, -side)]
    relayed = [me, at_place(0, side), across, at_place(1, side)]
    target = [onward if m else across for m in MODES]
    origin = [source if m else across for m in MODES]
    direct = [by_column if m else by_plane for m in MODES]
    relay = [relayed if m else by_plane for m in MODES]
    if MODES[2] == 0:
        relay[2] = [me, at_place(0, -1), at_place(0, 1), at_place(0, 2)]

    ids_copies = [
        remote(ids_b, idx.at[0], xsem_s.at[0], xsem_r.at[0], target[0]),
        remote(ids_b, idx.at[1], xsem_s.at[1], xsem_r.at[1], target[1]),
        remote(ids_f, idx.at[2], xsem_s.at[2], xsem_r.at[2], target[2]),
    ]
    share_copy = remote(share.at[0], share.at[1], xsem_s.at[3], xsem_r.at[3], target[1])

    pl.semaphore_wait(barrier, 9)
    raw_g = forward_raw(1, g, target[1])
    raw_b = forward_raw(0, norm.at[0], target[0])
    raw_f = forward_raw(2, norm.at[1], target[2])
    loads[1].wait()
    raw_g.start()
    for c in ids_copies:
        c.start()
    loads[0].wait()
    normalize(hb, norm.at[0], inv)
    raw_b.start()
    b0, b1 = ids_b[0:1, :], ids_b[1:2, :]
    f0, f1 = ids_f[0:1, :], ids_f[1:2, :]
    pack(0, 0, me, b0, b1, direct[0], norm.at[0])
    launch(0, 0, me, direct[0])
    for c in weights:
        c.start()

    scores, w0, w1 = route(ids_b, norm.at[0])
    small[0] = scores
    small[1] = jnp.broadcast_to(w0, (E, T))
    small[2] = jnp.broadcast_to(w1, (E, T))
    share[0, 0:1, :] = ROUTE_SCALE * w0
    share[0, 1:2, :] = ROUTE_SCALE * w1
    share_copy.start()
    pack(1, 0, me, b0, b1, direct[1], g, (ROUTE_SCALE * w0, ROUTE_SCALE * w1))
    launch(1, 0, me, direct[1])

    loads[2].wait()
    normalize(hf, norm.at[1], None)

    ids_copies[1].wait_recv()
    share_copy.wait_recv()
    raw_g.wait_recv()
    pack(
        1, 1, origin[1], idx[1, 0:1, :], idx[1, 1:2, :], relay[1], raw.at[1],
        (share[1, 0:1, :], share[1, 1:2, :]),
    )
    launch(1, 1, origin[1], relay[1])

    pack(2, 0, me, f0, f1, direct[2], norm.at[1])
    _, w0, w1 = route(ids_f, norm.at[1])
    eid, placed = places(f0, f1, list(range(E)))
    w = jnp.transpose(jnp.concatenate(
        weighted(placed, f0, f1, eid, ROUTE_SCALE * w0, ROUTE_SCALE * w1), axis=0
    ))
    hi = w.astype(BF16)
    wmat_f[0:T, :] = hi
    wmat_f[T:2 * T, :] = (w - hi.astype(F32)).astype(BF16)
    _, placed = places(b0, b1, list(range(E)))
    placed = jnp.concatenate(placed, axis=0)
    pmat[...] = placed.astype(BF16)
    wmat_b[...] = jnp.transpose(placed).astype(BF16)

    ids_copies[0].wait_recv()
    raw_b.wait_recv()
    pack(0, 1, origin[0], idx[0, 0:1, :], idx[0, 1:2, :], relay[0], raw.at[0])
    launch(0, 1, origin[0], relay[0])

    raw_f.start()
    launch(2, 0, me, direct[2])

    for c in weights:
        c.wait()
    packed_all(1).wait_recv()

    def d_act(i, c):
        at = cols(i, 256)
        dact[:, at] = dot_t(recv[1], down[pl.ds(pl.multiple_of(i * 256, 256), 256), :])
        return c

    lax.fori_loop(0, F // 256, d_act, 0)
    packed_all(0).wait_recv()
    dacc[...] = jnp.zeros_like(dacc)

    def hidden_grad(i, c):
        at = cols(i, 256)
        a = dot(recv[0], gate[:, at])
        b = dot(recv[0], up[:, at])
        da = dact[:, at]
        sg = jax.nn.sigmoid(a)
        silu = a * sg
        live = silu * b * da
        dacc[...] += live[:, 0:128] + live[:, 128:256]
        dab[:, at] = (da * b * sg * (1.0 + a * (1.0 - sg))).astype(BF16)
        dab[:, pl.ds(pl.multiple_of(F + i * 256, 128), 256)] = (da * silu).astype(BF16)
        return c

    lax.fori_loop(0, F // 256, hidden_grad, 0)

    ids_copies[2].wait_recv()
    raw_f.wait_recv()
    pack(2, 1, origin[2], idx[2, 0:1, :], idx[2, 1:2, :], relay[2], raw.at[2])
    launch(2, 1, origin[2], relay[2])

    for e in range(E):
        column = jnp.sum(dacc[e * CAP:(e + 1) * CAP, :], axis=1, keepdims=True)
        dots[e] = jnp.broadcast_to(jnp.sum(column * eye48, axis=0, keepdims=True), (E, T))
    for e in back_peers:
        remote(dots.at[e], dotr.at[me], tsem_s, tsem_r, e).start()
    dotr[me] = dots[me]

    def d_rows(i, c):
        at = pl.ds(pl.multiple_of(i * 256, 256), 256)
        recv[0, :, cols(i, 256)] = (
            dot_t(dab[:, 0:F], gate[at, :]) + dot_t(dab[:, F:2 * F], up[at, :])
        ).astype(BF16)
        return c

    for chunk in range(BACK_CHUNKS):
        each = BACK_WIDTH // 256
        lax.fori_loop(chunk * each, (chunk + 1) * each, d_rows, 0)
        at = pl.ds(chunk * BACK_WIDTH, BACK_WIDTH)
        for e in back_peers:
            remote(
                recv.at[0, block(e), at], retb.at[block(me), at],
                bsem_s.at[chunk], bsem_r.at[chunk], e,
            ).start()
        retb[block(me), at] = recv[0, block(me), at]

    packed_all(2).wait_recv()

    def hidden(i, c):
        at = cols(i, 256)
        a = dot(recv[2], gate[:, at])
        b = dot(recv[2], up[:, at])
        act[:, at] = (a * jax.nn.sigmoid(a) * b).astype(BF16)
        return c

    lax.fori_loop(0, F // 256, hidden, 0)

    for chunk in range(OUT_CHUNKS):
        at = pl.ds(chunk * OUT_WIDTH, OUT_WIDTH)
        recv[1, :, at] = dot(act[...], down[:, at]).astype(BF16)
        for e in out_peers:
            remote(
                recv.at[1, block(e), at], retf.at[block(me), at],
                fsem_s.at[chunk], fsem_r.at[chunk], e,
            ).start()
        retf[block(me), at] = recv[1, block(me), at]

    seven = pl.ds(0, 7 * CAP)
    all_dots = remote(dots.at[pl.ds(0, 7)], dotr.at[pl.ds(0, 7)], tsem_s, tsem_r, across)
    all_dots.wait_recv()
    scores = small[0]
    w0, w1 = small[1, 0:1, :], small[2, 0:1, :]
    d0 = jnp.zeros((1, T), F32)
    d1 = jnp.zeros((1, T), F32)
    for e in range(E):
        column = jnp.sum(dotr[e, 0:1, :] * eye48, axis=1, keepdims=True)
        value = jnp.sum(
            pmat[e * CAP:(e + 1) * CAP, :].astype(F32) * column, axis=0, keepdims=True
        )
        d0 = d0 + jnp.where(b0 == e, value, 0.0)
        d1 = d1 + jnp.where(b1 == e, value, 0.0)
    mean = d0 + d1
    d_logits = (
        jnp.where(expert8 == b0, d0 - w0 * mean, 0.0) + jnp.where(expert8 == b1, d1 - w1 * mean, 0.0)
    ) * (1.0 - scores)
    d_logits = jnp.transpose(
        jnp.concatenate([d_logits, jnp.zeros((T - E, T), F32)], axis=0)
    )[:, 0:E].astype(BF16)

    def all_back(chunk):
        at = pl.ds(chunk * BACK_WIDTH, BACK_WIDTH)
        return remote(
            recv.at[0, seven, at], retb.at[seven, at], bsem_s.at[chunk], bsem_r.at[chunk], across
        )

    def all_out(chunk):
        at = pl.ds(chunk * OUT_WIDTH, OUT_WIDTH)
        return remote(
            recv.at[1, seven, at], retf.at[seven, at], fsem_s.at[chunk], fsem_r.at[chunk], across
        )

    total_uh = jnp.zeros((T, 1), F32)
    for chunk in range(BACK_CHUNKS):
        all_back(chunk).wait_recv()
        for part in range(1):
            at = pl.ds(chunk * BACK_WIDTH + part * BACK_WIDTH, BACK_WIDTH)
            d_normed = dot(wmat_b[...], retb[:, at]) + dot(d_logits, router[:, at])
            scaled = gain[:, at] * d_normed
            u[:, at] = scaled
            total_uh = total_uh + jnp.sum(scaled * hb[:, at].astype(F32), axis=1, keepdims=True)
    r = inv[:, 0:1]
    pull = r * r * r * total_uh * (1.0 / D)

    def next_copy(at, out, stage, ssem, rsem, target):
        return pltpu.make_async_remote_copy(
            src_ref=stage.at[:, at], dst_ref=out.at[:, at], send_sem=ssem, recv_sem=rsem,
            device_id={"section": target}, device_id_type=MESH,
        )

    for chunk in range(OUT_CHUNKS):
        at = pl.ds(chunk * OUT_WIDTH, OUT_WIDTH)
        stage_b[:, at] = (
            g[:, at].astype(F32) + r * u[:, at] - hb[:, at].astype(F32) * pull
        ).astype(BF16)
        next_copy(at, outb_hbm, stage_b, pb_s, pb_r, behind).start()

    for chunk in range(OUT_CHUNKS):
        at = pl.ds(chunk * OUT_WIDTH, OUT_WIDTH)
        all_out(chunk).wait_recv()
        both = dot(wmat_f[...], retf[:, at])
        stage_f[:, at] = (hf[:, at].astype(F32) + (both[0:T] + both[T:2 * T])).astype(BF16)
        next_copy(at, outf_hbm, stage_f, pf_s, pf_r, ahead).start()

    for c in [*ids_copies, share_copy, raw_g, raw_b, raw_f, all_dots]:
        c.wait_send()
    for flow in range(3):
        packed_all(flow).wait_send()
    for chunk in range(BACK_CHUNKS):
        all_back(chunk).wait_send()
    for chunk in range(OUT_CHUNKS):
        all_out(chunk).wait_send()
    every = pl.ds(0, D)
    next_copy(every, outb_hbm, stage_b, pb_s, pb_r, behind).wait()
    next_copy(every, outf_hbm, stage_f, pf_s, pf_r, ahead).wait()


def hand_over(a_in, b_in, a_out, b_out, held, isem, osem):
    rows = T // HAND_PARTS
    pairs = [
        (src.at[pl.ds(i * rows, rows)], dst.at[pl.ds(i * rows, rows)])
        for i in range(HAND_PARTS)
        for src, dst in ((a_in, a_out), (b_in, b_out))
    ]
    ins = [pltpu.make_async_copy(s, held.at[i], isem.at[i]) for i, (s, _) in enumerate(pairs)]
    outs = [pltpu.make_async_copy(held.at[i], d, osem.at[i]) for i, (_, d) in enumerate(pairs)]
    for c in ins:
        c.start()
    for i, c in enumerate(outs):
        ins[i].wait()
        c.start()
    for c in outs:
        c.wait()


def local(
    fwd_input, bwd_input, bwd_grad, fwd_ids, bwd_ids, norm_gain, router, gate_w, up_w, down_w
):
    vmem = pl.BlockSpec(memory_space=pltpu.VMEM)
    hbm = pl.BlockSpec(memory_space=pl.ANY)
    dma = pltpu.SemaphoreType.DMA
    out = jax.ShapeDtypeStruct((T, D), BF16)
    fwd_next, bwd_prev = pl.pallas_call(
        kernel,
        out_shape=(out, out),
        in_specs=[vmem] * 4 + [hbm] * 6,
        out_specs=(hbm, hbm),
        scratch_shapes=[
            pltpu.VMEM((D, F), BF16), pltpu.VMEM((D, F), BF16), pltpu.VMEM((F, D), BF16),
            pltpu.VMEM((T, D), BF16), pltpu.VMEM((T, D), BF16), pltpu.VMEM((T, D), BF16),
            pltpu.VMEM((3, 6 * CAP, D), BF16), pltpu.VMEM((3, S, D), BF16), pltpu.VMEM((3, T, D), BF16),
            pltpu.VMEM((S, D), BF16), pltpu.VMEM((S, D), BF16), pltpu.VMEM((2, T, D), BF16),
            pltpu.VMEM((S, T), BF16), pltpu.VMEM((4 * CAP, T), BF16), pltpu.VMEM((4 * CAP, 128), F32),
            pltpu.VMEM((T, S), BF16), pltpu.VMEM((2 * T, S), BF16),
            pltpu.VMEM((S, F), F32), pltpu.VMEM((S, 2 * F), BF16), pltpu.VMEM((S, F), BF16),
            pltpu.VMEM((S, 128), F32), pltpu.VMEM((E, E, T), F32), pltpu.VMEM((E, E, T), F32),
            pltpu.VMEM((T, D), F32), pltpu.VMEM((T, D), BF16), pltpu.VMEM((T, D), BF16),
            pltpu.VMEM((T, 128), F32), pltpu.VMEM((3, E, T), F32),
            pltpu.VMEM((3, 2, T), jnp.int32), pltpu.VMEM((2, E, T), F32),
            dma((3,)), dma((3,)), dma((4,)), dma((4,)), dma((3,)), dma((3,)), dma((3,)), dma((3,)),
            dma((BACK_CHUNKS,)), dma((BACK_CHUNKS,)), dma, dma,
            dma((OUT_CHUNKS,)), dma((OUT_CHUNKS,)), dma, dma, dma, dma,
        ],
        compiler_params=pltpu.CompilerParams(
            collective_id=0, has_side_effects=True, vmem_limit_bytes=67043328
        ),
    )(
        fwd_ids[0].T, bwd_ids[0].T, norm_gain, router[0].T,
        fwd_input[0], bwd_input[0], bwd_grad[0], gate_w[0, 0], up_w[0, 0], down_w[0, 0],
    )
    parts = 2 * HAND_PARTS
    fwd_next, bwd_prev = pl.pallas_call(
        hand_over,
        out_shape=(out, out),
        in_specs=[hbm, hbm],
        out_specs=(hbm, hbm),
        scratch_shapes=[
            pltpu.VMEM((parts, T // HAND_PARTS, D), BF16), dma((parts,)), dma((parts,)),
        ],
    )(fwd_next, bwd_prev)
    return (fwd_next[None], bwd_prev[None])


def solution(mesh):
    placed = (
        P("section", "ep", None),
        P("section", "ep", None),
        P("section", "ep", None),
        P("section", "ep", None),
        P("section", "ep", None),
        P("section", None),
        P("section", None, None),
        P("section", "ep", None, None),
        P("section", "ep", None, None),
        P("section", "ep", None, None),
    )
    return jax.shard_map(
        local,
        mesh=mesh,
        in_specs=placed,
        out_specs=(P("section", "ep", None), P("section", "ep", None)),
        check_vma=False,
    )
```

```python
import jax
import jax.numpy as jnp
from jax import lax
from jax.experimental import pallas as pl
from jax.experimental.pallas import tpu as pltpu
from jax.sharding import PartitionSpec as P

NORM_EPSILON = 1e-06
ROUTE_SCALE = 2.5

D = 3584
F = 1024
T = 128
E = 8
CAP = 48
S = E * CAP
NEP = 8
NSEC = 16
MODES = (0, 1, 0)
BACK_ORDER = ((0, 2), (1, 0), (1, -1), (1, 1), (0, 1), (1, 2), (0, -1))
OUT_ORDER = ((0, 1), (1, 0), (0, -1), (1, 1), (0, 2), (1, -1), (1, 2))

BACK_CHUNKS = 7
BACK_WIDTH = D // BACK_CHUNKS
OUT_CHUNKS = 4
OUT_WIDTH = D // OUT_CHUNKS

HAND_PARTS = 4

MESH = pl.DeviceIdType.MESH
F32 = jnp.float32
BF16 = jnp.bfloat16


def dot(a, b):
    return jnp.dot(a, b, preferred_element_type=F32)


def dot_t(a, b):
    return lax.dot_general(a, b, (((1,), (1,)), ((), ())), preferred_element_type=F32)


def cols(i, width):
    return pl.ds(pl.multiple_of(i * width, 128), width)


def block(i):
    return pl.ds(pl.multiple_of(i * CAP, 16), CAP)


def kernel(
    ids_f, ids_b, gain, router, hf_hbm, hb_hbm, g_hbm, gate_hbm, up_hbm, down_hbm,
    outf_hbm, outb_hbm,
    gate, up, down, hf, hb, g,
    send, recv, raw, retb, retf, norm, pmat, qmat, scale, wmat_b, wmat_f,
    dact, dab, act, dacc, dots, dotr, u, stage_f, stage_b, inv, small, idx, share,
    wsem, isem, xsem_s, xsem_r, rsem_s, rsem_r, dsem_s, dsem_r, bsem_s, bsem_r, tsem_s, tsem_r,
    fsem_s, fsem_r, pf_s, pf_r, pb_s, pb_r,
):
    sec = lax.axis_index("section")
    me = lax.axis_index("ep")
    mx, mz = lax.rem(me, 4), me // 4
    side = 1 - 2 * lax.rem(sec, 2)

    def at_place(dz, dx):
        return lax.rem(mz + dz, 2) * 4 + lax.rem(mx + dx + 4, 4)

    back_peers = [at_place(dz, side * dx) for dz, dx in BACK_ORDER]
    out_peers = [at_place(dz, side * dx) for dz, dx in OUT_ORDER]
    across = at_place(1, 0)
    onward, source = at_place(0, side), at_place(0, -side)
    ahead, behind = lax.rem(sec + 1, NSEC), lax.rem(sec + NSEC - 1, NSEC)

    barrier = pltpu.get_barrier_semaphore()
    for e in back_peers:
        pl.semaphore_signal(barrier, 1, device_id={"ep": e}, device_id_type=MESH)
    for s in (ahead, behind):
        pl.semaphore_signal(barrier, 1, device_id={"section": s}, device_id_type=MESH)

    loads = [
        pltpu.make_async_copy(src, dst, isem.at[i])
        for i, (src, dst) in enumerate(((hb_hbm, hb), (g_hbm, g), (hf_hbm, hf)))
    ]
    weights = [
        pltpu.make_async_copy(src, dst, wsem.at[i])
        for i, (src, dst) in enumerate(((down_hbm, down), (gate_hbm, gate), (up_hbm, up)))
    ]
    for c in (loads[1], loads[0], loads[2]):
        c.start()

    def remote(src, dst, ssem, rsem, e):
        return pltpu.make_async_remote_copy(
            src_ref=src, dst_ref=dst, send_sem=ssem, recv_sem=rsem,
            device_id={"ep": e}, device_id_type=MESH,
        )

    row16 = lax.broadcasted_iota(jnp.int32, (16, T), 0)
    slot48 = lax.broadcasted_iota(jnp.int32, (CAP, T), 0).astype(F32)
    eye48 = (
        lax.broadcasted_iota(jnp.int32, (CAP, T), 0) == lax.broadcasted_iota(jnp.int32, (CAP, T), 1)
    ).astype(F32)
    earlier = (
        lax.broadcasted_iota(jnp.int32, (T, T), 0) < lax.broadcasted_iota(jnp.int32, (T, T), 1)
    ).astype(BF16)

    def places(ids0, ids1, order):
        eid = jnp.full((16, T), -1, jnp.int32)
        for k, e in enumerate(order):
            eid = jnp.where(row16 == k, e, eid)
        named = ((ids0 == eid) | (ids1 == eid)).astype(F32)
        rank = dot(named.astype(BF16), earlier)
        return eid, [
            jnp.where((slot48 == rank[k:k + 1, :]) & (named[k:k + 1, :] > 0.5), 1.0, 0.0)
            for k in range(len(order))
        ]

    def weighted(placed, ids0, ids1, eid, w0, w1):
        per = jnp.where(ids0 == eid, w0, 0.0) + jnp.where(ids1 == eid, w1, 0.0)
        return [p * per[k:k + 1, :] for k, p in enumerate(placed)]

    def pack(flow, half, owner, ids0, ids1, order, rows, w=None):
        eid, placed = places(ids0, ids1, order)
        qmat[...] = jnp.concatenate(placed, axis=0).astype(BF16)
        if w is not None:
            per = jnp.concatenate(weighted(placed, ids0, ids1, eid, w[0], w[1]), axis=0)
            scale[...] = jnp.broadcast_to(jnp.sum(per, axis=1, keepdims=True), (4 * CAP, 128))

        def step(i, c):
            at = cols(i, 512)
            packed = dot(qmat[...], rows[:, at])
            if w is not None:
                packed = scale[:, 0:1] * packed
            packed = packed.astype(BF16)
            recv[flow, block(owner), at] = packed[0:CAP]
            send[flow, half * 3 * CAP:(half + 1) * 3 * CAP, at] = packed[CAP:4 * CAP]
            return c

        lax.fori_loop(0, D // 512, step, 0)

    def launch(flow, half, owner, order):
        for k, e in enumerate(order[1:]):
            remote(
                send.at[flow, pl.ds((half * 3 + k) * CAP, CAP)], recv.at[flow, block(owner)],
                dsem_s.at[flow], dsem_r.at[flow], e,
            ).start()

    def packed_all(flow):
        part = pl.ds(0, 6 * CAP)
        return remote(
            send.at[flow, part], recv.at[flow, part], dsem_s.at[flow], dsem_r.at[flow], across
        )

    def forward_raw(flow, rows, e):
        return remote(rows, raw.at[flow], rsem_s.at[flow], rsem_r.at[flow], e)

    def normalize(rows, into, keep):
        def step(i, c):
            at = pl.ds(pl.multiple_of(i * 16, 16), 16)
            x = rows[at, :].astype(F32)
            r = lax.rsqrt(jnp.mean(x * x, axis=1, keepdims=True) + NORM_EPSILON)
            if keep is not None:
                keep[at, :] = jnp.broadcast_to(r, (16, 128))
            into[at, :] = (x * r * gain[...]).astype(BF16)
            return c

        lax.fori_loop(0, T // 16, step, 0)

    expert8 = lax.broadcasted_iota(jnp.int32, (E, T), 0)

    def route(ids, rows):
        scores = jax.nn.sigmoid(dot_t(router[...], rows[...]))
        s0 = jnp.sum(jnp.where(expert8 == ids[0:1, :], scores, 0.0), axis=0, keepdims=True)
        s1 = jnp.sum(jnp.where(expert8 == ids[1:2, :], scores, 0.0), axis=0, keepdims=True)
        total = s0 + s1
        return scores, s0 / total, s1 / total

    by_plane = [me, at_place(0, side), at_place(0, -side), at_place(0, 2)]
    by_column = [me, at_place(0, -side), across, at_place(1, -side)]
    relayed = [me, at_place(0, side), across, at_place(1, side)]
    target = [onward if m else across for m in MODES]
    origin = [source if m else across for m in MODES]
    direct = [by_column if m else by_plane for m in MODES]
    relay = [relayed if m else by_plane for m in MODES]
    if MODES[2] == 0:
        relay[2] = [me, at_place(0, -1), at_place(0, 1), at_place(0, 2)]

    ids_copies = [
        remote(ids_b, idx.at[0], xsem_s.at[0], xsem_r.at[0], target[0]),
        remote(ids_b, idx.at[1], xsem_s.at[1], xsem_r.at[1], target[1]),
        remote(ids_f, idx.at[2], xsem_s.at[2], xsem_r.at[2], target[2]),
    ]
    share_copy = remote(share.at[0], share.at[1], xsem_s.at[3], xsem_r.at[3], target[1])

    pl.semaphore_wait(barrier, 9)
    raw_g = forward_raw(1, g, target[1])
    raw_b = forward_raw(0, norm.at[0], target[0])
    raw_f = forward_raw(2, norm.at[1], target[2])
    loads[1].wait()
    raw_g.start()
    for c in ids_copies:
        c.start()
    loads[0].wait()
    normalize(hb, norm.at[0], inv)
    raw_b.start()
    b0, b1 = ids_b[0:1, :], ids_b[1:2, :]
    f0, f1 = ids_f[0:1, :], ids_f[1:2, :]
    pack(0, 0, me, b0, b1, direct[0], norm.at[0])
    launch(0, 0, me, direct[0])
    for c in weights:
        c.start()

    scores, w0, w1 = route(ids_b, norm.at[0])
    small[0] = scores
    small[1] = jnp.broadcast_to(w0, (E, T))
    small[2] = jnp.broadcast_to(w1, (E, T))
    share[0, 0:1, :] = ROUTE_SCALE * w0
    share[0, 1:2, :] = ROUTE_SCALE * w1
    share_copy.start()
    pack(1, 0, me, b0, b1, direct[1], g, (ROUTE_SCALE * w0, ROUTE_SCALE * w1))
    launch(1, 0, me, direct[1])

    loads[2].wait()
    normalize(hf, norm.at[1], None)

    ids_copies[1].wait_recv()
    share_copy.wait_recv()
    raw_g.wait_recv()
    pack(
        1, 1, origin[1], idx[1, 0:1, :], idx[1, 1:2, :], relay[1], raw.at[1],
        (share[1, 0:1, :], share[1, 1:2, :]),
    )
    launch(1, 1, origin[1], relay[1])

    pack(2, 0, me, f0, f1, direct[2], norm.at[1])
    ids_copies[0].wait_recv()
    raw_b.wait_recv()
    pack(0, 1, origin[0], idx[0, 0:1, :], idx[0, 1:2, :], relay[0], raw.at[0])
    launch(0, 1, origin[0], relay[0])

    raw_f.start()
    launch(2, 0, me, direct[2])
    _, w0, w1 = route(ids_f, norm.at[1])
    eid, placed = places(f0, f1, list(range(E)))
    w = jnp.transpose(jnp.concatenate(
        weighted(placed, f0, f1, eid, ROUTE_SCALE * w0, ROUTE_SCALE * w1), axis=0
    ))
    hi = w.astype(BF16)
    wmat_f[0:T, :] = hi
    wmat_f[T:2 * T, :] = (w - hi.astype(F32)).astype(BF16)
    _, placed = places(b0, b1, list(range(E)))
    placed = jnp.concatenate(placed, axis=0)
    pmat[...] = placed.astype(BF16)
    wmat_b[...] = jnp.transpose(placed).astype(BF16)


    for c in weights:
        c.wait()
    packed_all(1).wait_recv()

    def d_act(i, c):
        at = cols(i, 256)
        dact[:, at] = dot_t(recv[1], down[pl.ds(pl.multiple_of(i * 256, 256), 256), :])
        return c

    lax.fori_loop(0, F // 256, d_act, 0)
    packed_all(0).wait_recv()
    dacc[...] = jnp.zeros_like(dacc)

    def hidden_grad(i, c):
        at = cols(i, 256)
        a = dot(recv[0], gate[:, at])
        b = dot(recv[0], up[:, at])
        da = dact[:, at]
        sg = jax.nn.sigmoid(a)
        silu = a * sg
        live = silu * b * da
        dacc[...] += live[:, 0:128] + live[:, 128:256]
        dab[:, at] = (da * b * sg * (1.0 + a * (1.0 - sg))).astype(BF16)
        dab[:, pl.ds(pl.multiple_of(F + i * 256, 128), 256)] = (da * silu).astype(BF16)
        return c

    lax.fori_loop(0, F // 256, hidden_grad, 0)

    ids_copies[2].wait_recv()
    raw_f.wait_recv()
    pack(2, 1, origin[2], idx[2, 0:1, :], idx[2, 1:2, :], relay[2], raw.at[2])
    launch(2, 1, origin[2], relay[2])

    for e in range(E):
        column = jnp.sum(dacc[e * CAP:(e + 1) * CAP, :], axis=1, keepdims=True)
        dots[e] = jnp.broadcast_to(jnp.sum(column * eye48, axis=0, keepdims=True), (E, T))
    for e in back_peers:
        remote(dots.at[e], dotr.at[me], tsem_s, tsem_r, e).start()
    dotr[me] = dots[me]

    def d_rows(i, c):
        at = pl.ds(pl.multiple_of(i * 256, 256), 256)
        recv[0, :, cols(i, 256)] = (
            dot_t(dab[:, 0:F], gate[at, :]) + dot_t(dab[:, F:2 * F], up[at, :])
        ).astype(BF16)
        return c

    for chunk in range(BACK_CHUNKS):
        each = BACK_WIDTH // 256
        lax.fori_loop(chunk * each, (chunk + 1) * each, d_rows, 0)
        at = pl.ds(chunk * BACK_WIDTH, BACK_WIDTH)
        for e in back_peers:
            remote(
                recv.at[0, block(e), at], retb.at[block(me), at],
                bsem_s.at[chunk], bsem_r.at[chunk], e,
            ).start()
        retb[block(me), at] = recv[0, block(me), at]

    packed_all(2).wait_recv()

    def hidden(i, c):
        at = cols(i, 256)
        a = dot(recv[2], gate[:, at])
        b = dot(recv[2], up[:, at])
        act[:, at] = (a * jax.nn.sigmoid(a) * b).astype(BF16)
        return c

    lax.fori_loop(0, F // 256, hidden, 0)

    for chunk in range(OUT_CHUNKS):
        at = pl.ds(chunk * OUT_WIDTH, OUT_WIDTH)
        recv[1, :, at] = dot(act[...], down[:, at]).astype(BF16)
        for e in out_peers:
            remote(
                recv.at[1, block(e), at], retf.at[block(me), at],
                fsem_s.at[chunk], fsem_r.at[chunk], e,
            ).start()
        retf[block(me), at] = recv[1, block(me), at]

    seven = pl.ds(0, 7 * CAP)
    all_dots = remote(dots.at[pl.ds(0, 7)], dotr.at[pl.ds(0, 7)], tsem_s, tsem_r, across)
    all_dots.wait_recv()
    scores = small[0]
    w0, w1 = small[1, 0:1, :], small[2, 0:1, :]
    d0 = jnp.zeros((1, T), F32)
    d1 = jnp.zeros((1, T), F32)
    for e in range(E):
        column = jnp.sum(dotr[e, 0:1, :] * eye48, axis=1, keepdims=True)
        value = jnp.sum(
            pmat[e * CAP:(e + 1) * CAP, :].astype(F32) * column, axis=0, keepdims=True
        )
        d0 = d0 + jnp.where(b0 == e, value, 0.0)
        d1 = d1 + jnp.where(b1 == e, value, 0.0)
    mean = d0 + d1
    d_logits = (
        jnp.where(expert8 == b0, d0 - w0 * mean, 0.0) + jnp.where(expert8 == b1, d1 - w1 * mean, 0.0)
    ) * (1.0 - scores)
    d_logits = jnp.transpose(
        jnp.concatenate([d_logits, jnp.zeros((T - E, T), F32)], axis=0)
    )[:, 0:E].astype(BF16)

    def all_back(chunk):
        at = pl.ds(chunk * BACK_WIDTH, BACK_WIDTH)
        return remote(
            recv.at[0, seven, at], retb.at[seven, at], bsem_s.at[chunk], bsem_r.at[chunk], across
        )

    def all_out(chunk):
        at = pl.ds(chunk * OUT_WIDTH, OUT_WIDTH)
        return remote(
            recv.at[1, seven, at], retf.at[seven, at], fsem_s.at[chunk], fsem_r.at[chunk], across
        )

    total_uh = jnp.zeros((T, 1), F32)
    for chunk in range(BACK_CHUNKS):
        all_back(chunk).wait_recv()
        for part in range(1):
            at = pl.ds(chunk * BACK_WIDTH + part * BACK_WIDTH, BACK_WIDTH)
            d_normed = dot(wmat_b[...], retb[:, at]) + dot(d_logits, router[:, at])
            scaled = gain[:, at] * d_normed
            u[:, at] = scaled
            total_uh = total_uh + jnp.sum(scaled * hb[:, at].astype(F32), axis=1, keepdims=True)
    r = inv[:, 0:1]
    pull = r * r * r * total_uh * (1.0 / D)

    def next_copy(at, out, stage, ssem, rsem, target):
        return pltpu.make_async_remote_copy(
            src_ref=stage.at[:, at], dst_ref=out.at[:, at], send_sem=ssem, recv_sem=rsem,
            device_id={"section": target}, device_id_type=MESH,
        )

    for chunk in range(OUT_CHUNKS):
        at = pl.ds(chunk * OUT_WIDTH, OUT_WIDTH)
        stage_b[:, at] = (
            g[:, at].astype(F32) + r * u[:, at] - hb[:, at].astype(F32) * pull
        ).astype(BF16)
        next_copy(at, outb_hbm, stage_b, pb_s, pb_r, behind).start()

    for chunk in range(OUT_CHUNKS):
        at = pl.ds(chunk * OUT_WIDTH, OUT_WIDTH)
        all_out(chunk).wait_recv()
        both = dot(wmat_f[...], retf[:, at])
        stage_f[:, at] = (hf[:, at].astype(F32) + (both[0:T] + both[T:2 * T])).astype(BF16)
        next_copy(at, outf_hbm, stage_f, pf_s, pf_r, ahead).start()

    for c in [*ids_copies, share_copy, raw_g, raw_b, raw_f, all_dots]:
        c.wait_send()
    for flow in range(3):
        packed_all(flow).wait_send()
    for chunk in range(BACK_CHUNKS):
        all_back(chunk).wait_send()
    for chunk in range(OUT_CHUNKS):
        all_out(chunk).wait_send()
    every = pl.ds(0, D)
    next_copy(every, outb_hbm, stage_b, pb_s, pb_r, behind).wait()
    next_copy(every, outf_hbm, stage_f, pf_s, pf_r, ahead).wait()


def hand_over(a_in, b_in, a_out, b_out, held, isem, osem):
    rows = T // HAND_PARTS
    pairs = [
        (src.at[pl.ds(i * rows, rows)], dst.at[pl.ds(i * rows, rows)])
        for i in range(HAND_PARTS)
        for src, dst in ((a_in, a_out), (b_in, b_out))
    ]
    ins = [pltpu.make_async_copy(s, held.at[i], isem.at[i]) for i, (s, _) in enumerate(pairs)]
    outs = [pltpu.make_async_copy(held.at[i], d, osem.at[i]) for i, (_, d) in enumerate(pairs)]
    for c in ins:
        c.start()
    for i, c in enumerate(outs):
        ins[i].wait()
        c.start()
    for c in outs:
        c.wait()


def local(
    fwd_input, bwd_input, bwd_grad, fwd_ids, bwd_ids, norm_gain, router, gate_w, up_w, down_w
):
    vmem = pl.BlockSpec(memory_space=pltpu.VMEM)
    hbm = pl.BlockSpec(memory_space=pl.ANY)
    dma = pltpu.SemaphoreType.DMA
    out = jax.ShapeDtypeStruct((T, D), BF16)
    fwd_next, bwd_prev = pl.pallas_call(
        kernel,
        out_shape=(out, out),
        in_specs=[vmem] * 4 + [hbm] * 6,
        out_specs=(hbm, hbm),
        scratch_shapes=[
            pltpu.VMEM((D, F), BF16), pltpu.VMEM((D, F), BF16), pltpu.VMEM((F, D), BF16),
            pltpu.VMEM((T, D), BF16), pltpu.VMEM((T, D), BF16), pltpu.VMEM((T, D), BF16),
            pltpu.VMEM((3, 6 * CAP, D), BF16), pltpu.VMEM((3, S, D), BF16), pltpu.VMEM((3, T, D), BF16),
            pltpu.VMEM((S, D), BF16), pltpu.VMEM((S, D), BF16), pltpu.VMEM((2, T, D), BF16),
            pltpu.VMEM((S, T), BF16), pltpu.VMEM((4 * CAP, T), BF16), pltpu.VMEM((4 * CAP, 128), F32),
            pltpu.VMEM((T, S), BF16), pltpu.VMEM((2 * T, S), BF16),
            pltpu.VMEM((S, F), F32), pltpu.VMEM((S, 2 * F), BF16), pltpu.VMEM((S, F), BF16),
            pltpu.VMEM((S, 128), F32), pltpu.VMEM((E, E, T), F32), pltpu.VMEM((E, E, T), F32),
            pltpu.VMEM((T, D), F32), pltpu.VMEM((T, D), BF16), pltpu.VMEM((T, D), BF16),
            pltpu.VMEM((T, 128), F32), pltpu.VMEM((3, E, T), F32),
            pltpu.VMEM((3, 2, T), jnp.int32), pltpu.VMEM((2, E, T), F32),
            dma((3,)), dma((3,)), dma((4,)), dma((4,)), dma((3,)), dma((3,)), dma((3,)), dma((3,)),
            dma((BACK_CHUNKS,)), dma((BACK_CHUNKS,)), dma, dma,
            dma((OUT_CHUNKS,)), dma((OUT_CHUNKS,)), dma, dma, dma, dma,
        ],
        compiler_params=pltpu.CompilerParams(
            collective_id=0, has_side_effects=True, vmem_limit_bytes=67043328
        ),
    )(
        fwd_ids[0].T, bwd_ids[0].T, norm_gain, router[0].T,
        fwd_input[0], bwd_input[0], bwd_grad[0], gate_w[0, 0], up_w[0, 0], down_w[0, 0],
    )
    parts = 2 * HAND_PARTS
    fwd_next, bwd_prev = pl.pallas_call(
        hand_over,
        out_shape=(out, out),
        in_specs=[hbm, hbm],
        out_specs=(hbm, hbm),
        scratch_shapes=[
            pltpu.VMEM((parts, T // HAND_PARTS, D), BF16), dma((parts,)), dma((parts,)),
        ],
    )(fwd_next, bwd_prev)
    return (fwd_next[None], bwd_prev[None])


def solution(mesh):
    placed = (
        P("section", "ep", None),
        P("section", "ep", None),
        P("section", "ep", None),
        P("section", "ep", None),
        P("section", "ep", None),
        P("section", None),
        P("section", None, None),
        P("section", "ep", None, None),
        P("section", "ep", None, None),
        P("section", "ep", None, None),
    )
    return jax.shard_map(
        local,
        mesh=mesh,
        in_specs=placed,
        out_specs=(P("section", "ep", None), P("section", "ep", None)),
        check_vma=False,
    )
```
